32 devices in a mesh: gx: 8 (over z, y), gy: 4 (over x, core).
Axes of the slice: x: 2, y: 2, z: 4, core: 2. Of those that a mesh axis runs over, the one named last changes fastest.
Arguments:
- states: bfloat16 [80, 8, 256, 1024], P('gx', None, 'gy'), may hold values from -6 to 6
- obs_pert: bfloat16 [80, 4, 1024], P(None, 'gy', 'gx'), may hold values from -6 to 6
- obs_innov: bfloat16 [4, 1024], P('gy', 'gx'), may hold values from -6 to 6
- obs_cell: int32 [4, 1024], P('gy', 'gx'), may hold values from 0 to 8191
- obs_count: int32 [4, 8], P('gy', 'gx'), may hold values from 16 to 128, as said below
Outputs:
- analysis: bfloat16 [80, 8, 256, 1024], P(None, None, 'gy', 'gx')
The draws below stay inside these ranges and needn't reach their ends.
Inputs may be any that keep to these rules, and one draw needn't show every extreme that they name: `obs_count`: at most 128; some tile has exactly 128. `obs_cell`: slots at or after their tile's count are unused.
All inputs are finite; a program needn't handle non-finite values.
Results may differ from the reference program's by a relative error of at most 0.0057.
Values may be sent and summed in bfloat16 or wider, within the bound.
No kernel may reach another device: no remote copies, remote signals or barrier semaphores. Data moves between devices by JAX's collectives and lax.ppermute only.
A program may use at most 128 MiB of HBM per device.

```python
import jax
import jax.numpy as jnp
from jax import lax

K = 80
L = 8
TX = 128
TY = 64
OBS_DEV = 128
NS_ITERS = 4
NX = 1024
NY = 256
TILE_ROWS = 4
TILE_COLS = 8
OBS_COLS = 1024


def draw_obs_count(key, part):
    base = jax.random.randint(key, (TILE_ROWS * TILE_COLS,), OBS_DEV // 8, OBS_DEV + 1)
    spot = jax.random.randint(jax.random.fold_in(key, 7), (), 0, TILE_ROWS * TILE_COLS)
    flat = jnp.where(jnp.arange(TILE_ROWS * TILE_COLS) == spot, OBS_DEV, base)
    return flat.reshape(TILE_ROWS, TILE_COLS).astype(jnp.int32)


def plant(entries, own_key, least, top_value):
    extent = entries.shape
    index_at = [jax.random.randint(jax.random.fold_in(own_key, axis), (), 0, extent[axis]) for axis in range(len(extent))]
    entries = entries.at[tuple(index_at)].set(least)
    longest = extent.index(max(extent))
    index_at[longest] = (index_at[longest] + 1) % extent[longest]
    return entries.at[tuple(index_at)].set(top_value)


def block_levels(rng, extent, split, least, top_value):
    def one(axis_at, parts):
        draws = jax.random.uniform(jax.random.fold_in(jax.random.fold_in(rng, 6), axis_at), (parts,), jnp.float32, least / len(split), top_value / len(split))
        return jnp.repeat(jnp.exp(draws), extent[axis_at] // parts).reshape((-1,) + (1,) * (len(extent) - axis_at - 1))

    factor_of = one(*split[0])
    for cut in split[1:]:
        factor_of = factor_of * one(*cut)
    return factor_of


def noise(rng, extent, scale, most, cuts=(), kind=jnp.bfloat16):
    values = scale * jax.random.normal(rng, extent, jnp.float32)
    if cuts:
        values = values * block_levels(rng, extent, cuts, -0.22, 0.18)
    return jnp.clip(values, -most, most).astype(kind)


def setup_inputs(seed: int = 0) -> dict:
    streams_of = jax.random.split(jax.random.key(seed), 6)
    return {
        "states": noise(streams_of[0], (K, L, NY, NX), 1.0, 6.0, ((0, 8), (2, 4))),
        "obs_pert": noise(streams_of[1], (K, TILE_ROWS, OBS_COLS), 1.0, 6.0, ((1, 4), (2, 8))),
        "obs_innov": noise(streams_of[2], (TILE_ROWS, OBS_COLS), 1.0, 6.0, ((0, 4), (1, 8))),
        "obs_cell": plant(jax.random.randint(streams_of[3], (TILE_ROWS, OBS_COLS), 0, TY * TX), jax.random.fold_in(streams_of[3], 1), 0, (TY * TX) - 1).astype(jnp.int32),
        "obs_count": draw_obs_count(jax.random.fold_in(streams_of[5], 71), 0),
    }


def locality(groups, row_index, col_index, tile_rows, tile_cols):
    slot_count = groups.shape[1] // 9
    width_x = TX * tile_cols
    height_y = TY * tile_rows
    position = lax.broadcasted_iota(jnp.int32, (1, 9 * slot_count), 1)
    row_shift = position // (3 * slot_count) - 1
    col_shift = position // slot_count % 3 - 1
    folded = jnp.logical_and(row_index == tile_rows - 1, row_shift == 1)
    src_row = jnp.where(folded, tile_rows - 1, row_index + row_shift)
    src_col = jnp.where(folded, (tile_cols - 1 - col_index + col_shift) % tile_cols, (col_index + col_shift) % tile_cols)
    local_row = groups[-2:-1].astype(jnp.float32)
    local_col = groups[-1:].astype(jnp.float32)
    obs_y = src_row.astype(jnp.float32) * TY + local_row
    obs_x = src_col.astype(jnp.float32) * TX + local_col
    obs_y = jnp.where(folded, 2.0 * height_y - 1.0 - obs_y, obs_y)
    obs_x = jnp.where(folded, width_x - 1.0 - obs_x, obs_x)
    block_y = (row_index * TY + lax.broadcasted_iota(jnp.int32, (TY, 1), 0)).astype(jnp.float32)
    gap_y = obs_y - block_y
    offset = jnp.mod(obs_x - (col_index * TX).astype(jnp.float32), float(width_x))
    gap_x = jnp.where(offset < TX, 0.0, jnp.minimum(offset - (TX - 1.0), width_x - offset))
    radius = float(TY // 2)
    scaled = jnp.minimum(1.0, (gap_x * gap_x + gap_y * gap_y) / (radius * radius))
    return (1.0 - scaled) * (1.0 - scaled)

def batched(left, right):
    return jnp.einsum('bij,bjk->bik', left, right, precision=lax.Precision.HIGHEST)

def transforms(groups, taper, members):
    rows = groups[:members + 1]
    weighted = (rows.astype(jnp.float32)[None] * taper[:, None, :]).astype(jnp.bfloat16)
    products = jnp.einsum('bks,js->bkj', weighted.astype(jnp.float32), groups[:members].astype(jnp.float32))
    covariance = products[:, :members, :]
    projected = products[:, members, :]
    identity = jnp.eye(members, dtype=jnp.float32)
    system = identity[None] + covariance / (members - 1.0)
    norm_scale = jnp.sqrt(lax.optimization_barrier(jnp.sum(system * system, axis=(1, 2))))[:, None, None]
    iterate = system / norm_scale
    inverse = jnp.broadcast_to(identity, system.shape)
    for sweep in range(NS_ITERS):
        correction = 1.5 * identity[None] - 0.5 * batched(inverse, iterate)
        iterate = batched(iterate, correction)
        inverse = batched(correction, inverse)
    spread_weights = inverse / jnp.sqrt(norm_scale)
    mean_weights = batched(inverse, batched(inverse, projected[:, :, None])) / (norm_scale * (members - 1.0))
    return (spread_weights + mean_weights).astype(jnp.bfloat16)

def analysis_step(tile_states, transform):
    average = lax.optimization_barrier(jnp.mean(tile_states.astype(jnp.float32), axis=0))
    perturb = (tile_states.astype(jnp.float32) - average[None]).astype(jnp.bfloat16)
    mixed_members = jnp.einsum('klrx,rkj->jlrx', perturb.astype(jnp.float32), transform.astype(jnp.float32))
    return (average[None] + mixed_members).astype(jnp.bfloat16)

def reference(states, obs_pert, obs_innov, obs_cell, obs_count):
    tile_rows = TILE_ROWS
    tile_cols = TILE_COLS
    members = K
    filled = jnp.arange(OBS_DEV, dtype=jnp.int32)[None, None, :] < obs_count[:, :, None]
    perturbs = obs_pert.reshape(members, tile_rows, tile_cols, OBS_DEV)
    perturbs = jnp.where(filled[None], perturbs, jnp.zeros_like(perturbs))
    innovation = obs_innov.reshape(tile_rows, tile_cols, OBS_DEV)
    innovation = jnp.where(filled, innovation, jnp.zeros_like(innovation))
    obs_cells = obs_cell.reshape(tile_rows, tile_cols, OBS_DEV)
    packed = jnp.concatenate([perturbs, innovation[None], (obs_cells // TX).astype(jnp.bfloat16)[None], (obs_cells % TX).astype(jnp.bfloat16)[None]], axis=0)

    def one_tile(tile_index):
        row_index = tile_index // tile_cols
        col_index = tile_index % tile_cols
        pieces = []
        for row_shift in (-1, 0, 1):
            for col_shift in (-1, 0, 1):
                present = jnp.bool_(True)
                if row_shift == 1:
                    folded = row_index == tile_rows - 1
                    src_row = jnp.where(folded, tile_rows - 1, row_index + 1)
                    src_col = jnp.where(folded, (tile_cols - 1 - col_index + col_shift) % tile_cols, (col_index + col_shift) % tile_cols)
                elif row_shift == -1:
                    src_row = jnp.maximum(row_index - 1, 0)
                    src_col = (col_index + col_shift) % tile_cols
                    present = row_index > 0
                else:
                    src_row = row_index
                    src_col = (col_index + col_shift) % tile_cols
                neighbour = packed[:, src_row.astype(jnp.int32), src_col.astype(jnp.int32), :]
                pieces.append(jnp.where(present, neighbour, jnp.zeros_like(neighbour)))
        groups = jnp.concatenate(pieces, axis=1)
        taper = locality(groups, row_index, col_index, tile_rows, tile_cols)
        transform = transforms(groups, taper, members)
        tile_states = lax.dynamic_slice(states, (jnp.int32(0), jnp.int32(0), (row_index * TY).astype(jnp.int32), (col_index * TX).astype(jnp.int32)), (members, L, TY, TX))
        return analysis_step(tile_states, transform)
    tiles = lax.map(one_tile, jnp.arange(tile_rows * tile_cols, dtype=jnp.int32))
    tiles = tiles.reshape(tile_rows, tile_cols, members, L, TY, TX)
    return tiles.transpose(2, 3, 0, 4, 1, 5).reshape(members, L, TY * tile_rows, TX * tile_cols)
```

```python
import jax
import jax.numpy as jnp
from jax import lax
from jax.experimental import pallas as pl
from jax.experimental.pallas import tpu as pltpu
from jax.sharding import PartitionSpec as P

NS_ITERS = 4
ROWS = 16

def pack(states, count):
    members, levels, height, whole = states.shape
    rows = height // 2
    width = whole // count

    def kernel(in_ref, out_ref):
        for tile in range(count):
            out_ref[tile] = in_ref[:, :, :, tile * width : (tile + 1) * width]

    return pl.pallas_call(
        kernel,
        grid=(levels, 2),
        in_specs=[pl.BlockSpec((members, 1, rows, whole), lambda l, r: (0, l, r, 0))],
        out_specs=pl.BlockSpec((count, members, 1, rows, width), lambda l, r: (0, 0, l, r, 0)),
        out_shape=jax.ShapeDtypeStruct((count, members, levels, height, width), states.dtype),
        name="pack",
    )(states)


def analyse(tile_states, transposed):
    total, level_count, height, width = tile_states.shape
    pair = 2

    def kernel(trans_ref, in_ref, out_ref, work, mixed):
        means = []
        for level in range(pair):
            acc = jnp.zeros((ROWS, width), jnp.float32)
            for member in range(total):
                value = in_ref[member, level].astype(jnp.float32)
                acc = acc + value
                work[level, member * ROWS : (member + 1) * ROWS, :] = value
            means.append(acc / float(total))
        for row in range(ROWS):
            sides = [
                work[level, pl.ds(row, total, stride=ROWS), :] - means[level][row : row + 1]
                for level in range(pair)
            ]
            perturb = jnp.concatenate(sides, axis=1).astype(jnp.bfloat16)
            result = jnp.dot(trans_ref[row], perturb, preferred_element_type=jnp.float32)
            for level in range(pair):
                mixed[level, pl.ds(row, total, stride=ROWS), :] = (
                    result[:, level * width : (level + 1) * width] + means[level][row : row + 1]
                )
        for level in range(pair):
            out_ref[:, level] = mixed[level].reshape(total, ROWS, width).astype(out_ref.dtype)

    return pl.pallas_call(
        kernel,
        grid=(height // ROWS, level_count // pair),
        in_specs=[
            pl.BlockSpec((ROWS, total, total), lambda r, l: (r, 0, 0)),
            pl.BlockSpec((total, pair, ROWS, width), lambda r, l: (0, l, r, 0)),
        ],
        out_specs=pl.BlockSpec((total, pair, ROWS, width), lambda r, l: (0, l, r, 0)),
        scratch_shapes=[
            pltpu.VMEM((pair, total * ROWS, width), jnp.float32),
            pltpu.VMEM((pair, total * ROWS, width), jnp.float32),
        ],
        out_shape=jax.ShapeDtypeStruct(tile_states.shape, tile_states.dtype),
        name="analyse",
    )(transposed, tile_states)


def locality(groups, row_index, col_index, tile_rows, tile_cols, height, width):
    slot_count = groups.shape[1] // 9
    width_x = width * tile_cols
    height_y = height * tile_rows
    position = lax.broadcasted_iota(jnp.int32, (1, 9 * slot_count), 1)
    row_shift = position // (3 * slot_count) - 1
    col_shift = position // slot_count % 3 - 1
    folded = jnp.logical_and(row_index == tile_rows - 1, row_shift == 1)
    src_row = jnp.where(folded, tile_rows - 1, row_index + row_shift)
    src_col = jnp.where(
        folded,
        (tile_cols - 1 - col_index + col_shift) % tile_cols,
        (col_index + col_shift) % tile_cols,
    )
    local_row = groups[-2:-1].astype(jnp.float32)
    local_col = groups[-1:].astype(jnp.float32)
    obs_y = src_row.astype(jnp.float32) * height + local_row
    obs_x = src_col.astype(jnp.float32) * width + local_col
    obs_y = jnp.where(folded, 2.0 * height_y - 1.0 - obs_y, obs_y)
    obs_x = jnp.where(folded, width_x - 1.0 - obs_x, obs_x)
    block_y = (row_index * height + lax.broadcasted_iota(jnp.int32, (height, 1), 0)).astype(
        jnp.float32
    )
    gap_y = obs_y - block_y
    offset = jnp.mod(obs_x - (col_index * width).astype(jnp.float32), float(width_x))
    gap_x = jnp.where(offset < width, 0.0, jnp.minimum(offset - (width - 1.0), width_x - offset))
    radius = float(height // 2)
    scaled = jnp.minimum(1.0, (gap_x * gap_x + gap_y * gap_y) / (radius * radius))
    return (1.0 - scaled) * (1.0 - scaled)


def batched(left, right):
    return jnp.einsum("bij,bjk->bik", left, right, precision=lax.Precision.HIGHEST)


def transforms(groups, taper, members):
    rows = groups[: members + 1]
    weighted = (rows.astype(jnp.float32)[None] * taper[:, None, :]).astype(jnp.bfloat16)
    products = jnp.einsum(
        "bks,js->bkj", weighted, groups[:members], preferred_element_type=jnp.float32
    )
    covariance = products[:, :members, :]
    projected = products[:, members, :]
    identity = jnp.eye(members, dtype=jnp.float32)
    system = identity[None] + covariance / (members - 1.0)
    norm_scale = jnp.sqrt(jnp.sum(system * system, axis=(1, 2)))[:, None, None]
    iterate = system / norm_scale
    inverse = jnp.broadcast_to(identity, system.shape)
    for sweep in range(NS_ITERS):
        correction = 1.5 * identity[None] - 0.5 * batched(inverse, iterate)
        iterate = batched(iterate, correction)
        inverse = batched(correction, inverse)
    spread_weights = inverse / jnp.sqrt(norm_scale)
    mean_weights = batched(inverse, batched(inverse, projected[:, :, None])) / (
        norm_scale * (members - 1.0)
    )
    return (spread_weights + mean_weights).astype(jnp.bfloat16)


def gather_groups(obs_pert, obs_innov, obs_cell, obs_count, width):
    slot_count = obs_pert.shape[2]
    tile_cols = lax.axis_size("gx")
    tile_rows = lax.axis_size("gy")
    filled = lax.broadcasted_iota(jnp.int32, (1, slot_count), 1) < obs_count
    perturbs = obs_pert[:, 0, :]
    perturbs = jnp.where(filled, perturbs, jnp.zeros_like(perturbs))
    innovation = jnp.where(filled, obs_innov, jnp.zeros_like(obs_innov))
    packed = jnp.concatenate(
        [
            perturbs,
            innovation,
            (obs_cell // width).astype(jnp.bfloat16),
            (obs_cell % width).astype(jnp.bfloat16),
        ],
        axis=0,
    )
    east = [(i, (i + 1) % tile_cols) for i in range(tile_cols)]
    extended = jnp.concatenate(
        [
            lax.ppermute(packed, "gx", east),
            packed,
            lax.ppermute(packed, "gx", [(j, i) for i, j in east]),
        ],
        axis=1,
    )
    mirror = lax.ppermute(extended, "gx", [(i, tile_cols - 1 - i) for i in range(tile_cols)])
    north = [(i, i + 1) for i in range(tile_rows - 1)]
    south = lax.ppermute(extended, "gy", north)
    above = lax.ppermute(extended, "gy", [(j, i) for i, j in north])
    at_north = lax.axis_index("gy") == tile_rows - 1
    return jnp.concatenate([south, extended, jnp.where(at_north, mirror, above)], axis=1)


def body(states, obs_pert, obs_innov, obs_cell, obs_count):
    members = obs_pert.shape[0]
    tile_cols = lax.axis_size("gx")
    tile_rows = lax.axis_size("gy")
    levels, height = states.shape[1:3]
    width = states.shape[3] // tile_cols
    col_index = lax.axis_index("gx")
    row_index = lax.axis_index("gy")
    groups = gather_groups(obs_pert, obs_innov, obs_cell, obs_count, width)
    blocks = pack(states, tile_cols)
    groups, blocks = lax.optimization_barrier((groups, blocks))
    taper = locality(groups, row_index, col_index, tile_rows, tile_cols, height, width)
    transposed = jnp.swapaxes(transforms(groups, taper, members), 1, 2)
    tile_states = lax.all_to_all(blocks, "gx", split_axis=0, concat_axis=0, tiled=True)
    tile_states = tile_states.reshape(members, levels, height, width)
    return analyse(tile_states, transposed)


def solution(mesh):
    return jax.shard_map(
        body,
        mesh=mesh,
        in_specs=(
            P("gx", None, "gy", None),
            P(None, "gy", "gx"),
            P("gy", "gx"),
            P("gy", "gx"),
            P("gy", "gx"),
        ),
        out_specs=P(None, None, "gy", "gx"),
        check_vma=False,
    )
```

```python
import jax
import jax.numpy as jnp
from jax import lax
from jax.experimental import pallas as pl
from jax.experimental.pallas import tpu as pltpu
from jax.sharding import PartitionSpec as P

NS_ITERS = 4
ROWS = 16

def pack(states, count, first, span):
    members, _, height, whole = states.shape
    rows = height // 2
    width = whole // count

    def kernel(in_ref, out_ref):
        for tile in range(count):
            out_ref[tile] = in_ref[:, :, :, tile * width : (tile + 1) * width]

    return pl.pallas_call(
        kernel,
        grid=(span, 2),
        in_specs=[pl.BlockSpec((members, 1, rows, whole), lambda l, r: (0, l + first, r, 0))],
        out_specs=pl.BlockSpec((count, members, 1, rows, width), lambda l, r: (0, 0, l, r, 0)),
        out_shape=jax.ShapeDtypeStruct((count, members, span, height, width), states.dtype),
        name="pack",
    )(states)


def analyse(tile_states, transposed, previous, first, levels):
    total, level_count, height, width = tile_states.shape
    pair = 2

    def kernel(trans_ref, in_ref, *refs):
        out_ref, work, mixed = refs[-3:]
        means = []
        for level in range(pair):
            acc = jnp.zeros((ROWS, width), jnp.float32)
            for member in range(total):
                value = in_ref[member, level].astype(jnp.float32)
                acc = acc + value
                work[level, member * ROWS : (member + 1) * ROWS, :] = value
            means.append(acc / float(total))
        for row in range(ROWS):
            sides = [
                work[level, pl.ds(row, total, stride=ROWS), :] - means[level][row : row + 1]
                for level in range(pair)
            ]
            perturb = jnp.concatenate(sides, axis=1).astype(jnp.bfloat16)
            result = jnp.dot(trans_ref[row], perturb, preferred_element_type=jnp.float32)
            for level in range(pair):
                mixed[level, pl.ds(row, total, stride=ROWS), :] = (
                    result[:, level * width : (level + 1) * width] + means[level][row : row + 1]
                )
        for level in range(pair):
            out_ref[:, level] = mixed[level].reshape(total, ROWS, width).astype(out_ref.dtype)

    return pl.pallas_call(
        kernel,
        grid=(height // ROWS, level_count // pair),
        in_specs=[
            pl.BlockSpec((ROWS, total, total), lambda r, l: (r, 0, 0)),
            pl.BlockSpec((total, pair, ROWS, width), lambda r, l: (0, l, r, 0)),
        ]
        + [pl.BlockSpec(memory_space=pl.ANY)] * len(previous),
        out_specs=pl.BlockSpec(
            (total, pair, ROWS, width), lambda r, l: (0, l + first // pair, r, 0)
        ),
        input_output_aliases={2: 0} if previous else {},
        scratch_shapes=[
            pltpu.VMEM((pair, total * ROWS, width), jnp.float32),
            pltpu.VMEM((pair, total * ROWS, width), jnp.float32),
        ],
        out_shape=jax.ShapeDtypeStruct((total, levels, height, width), tile_states.dtype),
        name="analyse",
    )(transposed, tile_states, *previous)


def locality(groups, row_index, col_index, tile_rows, tile_cols, height, width):
    slot_count = groups.shape[1] // 9
    width_x = width * tile_cols
    height_y = height * tile_rows
    position = lax.broadcasted_iota(jnp.int32, (1, 9 * slot_count), 1)
    row_shift = position // (3 * slot_count) - 1
    col_shift = position // slot_count % 3 - 1
    folded = jnp.logical_and(row_index == tile_rows - 1, row_shift == 1)
    src_row = jnp.where(folded, tile_rows - 1, row_index + row_shift)
    src_col = jnp.where(
        folded,
        (tile_cols - 1 - col_index + col_shift) % tile_cols,
        (col_index + col_shift) % tile_cols,
    )
    local_row = groups[-2:-1].astype(jnp.float32)
    local_col = groups[-1:].astype(jnp.float32)
    obs_y = src_row.astype(jnp.float32) * height + local_row
    obs_x = src_col.astype(jnp.float32) * width + local_col
    obs_y = jnp.where(folded, 2.0 * height_y - 1.0 - obs_y, obs_y)
    obs_x = jnp.where(folded, width_x - 1.0 - obs_x, obs_x)
    block_y = (row_index * height + lax.broadcasted_iota(jnp.int32, (height, 1), 0)).astype(
        jnp.float32
    )
    gap_y = obs_y - block_y
    offset = jnp.mod(obs_x - (col_index * width).astype(jnp.float32), float(width_x))
    gap_x = jnp.where(offset < width, 0.0, jnp.minimum(offset - (width - 1.0), width_x - offset))
    radius = float(height // 2)
    scaled = jnp.minimum(1.0, (gap_x * gap_x + gap_y * gap_y) / (radius * radius))
    return (1.0 - scaled) * (1.0 - scaled)


def batched(left, right):
    return jnp.einsum("bij,bjk->bik", left, right, precision=lax.Precision.HIGHEST)


def transforms(groups, taper, members):
    rows = groups[: members + 1]
    weighted = (rows.astype(jnp.float32)[None] * taper[:, None, :]).astype(jnp.bfloat16)
    products = jnp.einsum(
        "bks,js->bkj", weighted, groups[:members], preferred_element_type=jnp.float32
    )
    covariance = products[:, :members, :]
    projected = products[:, members, :]
    identity = jnp.eye(members, dtype=jnp.float32)
    system = identity[None] + covariance / (members - 1.0)
    norm_scale = jnp.sqrt(jnp.sum(system * system, axis=(1, 2)))[:, None, None]
    iterate = system / norm_scale
    inverse = jnp.broadcast_to(identity, system.shape)
    for sweep in range(NS_ITERS):
        correction = 1.5 * identity[None] - 0.5 * batched(inverse, iterate)
        iterate = batched(iterate, correction)
        inverse = batched(correction, inverse)
    spread_weights = inverse / jnp.sqrt(norm_scale)
    mean_weights = batched(inverse, batched(inverse, projected[:, :, None])) / (
        norm_scale * (members - 1.0)
    )
    return (spread_weights + mean_weights).astype(jnp.bfloat16)


def gather_groups(obs_pert, obs_innov, obs_cell, obs_count, width):
    slot_count = obs_pert.shape[2]
    tile_cols = lax.axis_size("gx")
    tile_rows = lax.axis_size("gy")
    filled = lax.broadcasted_iota(jnp.int32, (1, slot_count), 1) < obs_count
    perturbs = obs_pert[:, 0, :]
    perturbs = jnp.where(filled, perturbs, jnp.zeros_like(perturbs))
    innovation = jnp.where(filled, obs_innov, jnp.zeros_like(obs_innov))
    packed = jnp.concatenate(
        [
            perturbs,
            innovation,
            (obs_cell // width).astype(jnp.bfloat16),
            (obs_cell % width).astype(jnp.bfloat16),
        ],
        axis=0,
    )
    east = [(i, (i + 1) % tile_cols) for i in range(tile_cols)]
    extended = jnp.concatenate(
        [
            lax.ppermute(packed, "gx", east),
            packed,
            lax.ppermute(packed, "gx", [(j, i) for i, j in east]),
        ],
        axis=1,
    )
    mirror = lax.ppermute(extended, "gx", [(i, tile_cols - 1 - i) for i in range(tile_cols)])
    north = [(i, i + 1) for i in range(tile_rows - 1)]
    south = lax.ppermute(extended, "gy", north)
    above = lax.ppermute(extended, "gy", [(j, i) for i, j in north])
    at_north = lax.axis_index("gy") == tile_rows - 1
    return jnp.concatenate([south, extended, jnp.where(at_north, mirror, above)], axis=1)


def body(states, obs_pert, obs_innov, obs_cell, obs_count):
    members = obs_pert.shape[0]
    tile_cols = lax.axis_size("gx")
    tile_rows = lax.axis_size("gy")
    levels, height = states.shape[1:3]
    width = states.shape[3] // tile_cols
    col_index = lax.axis_index("gx")
    row_index = lax.axis_index("gy")
    groups = gather_groups(obs_pert, obs_innov, obs_cell, obs_count, width)
    span = levels // 2
    early = pack(states, tile_cols, 0, span)
    groups, early = lax.optimization_barrier((groups, early))
    taper = locality(groups, row_index, col_index, tile_rows, tile_cols, height, width)
    transposed = jnp.swapaxes(transforms(groups, taper, members), 1, 2)
    late = pack(states, tile_cols, span, span)
    done = ()
    received = [
        lax.all_to_all(blocks, "gx", split_axis=0, concat_axis=0, tiled=True)
        for blocks in (early, late)
    ]
    for chunk, blocks in enumerate(received):
        blocks = blocks.reshape(members, span, height, width)
        done = (analyse(blocks, transposed, done, chunk * span, levels),)
    return done[0]


def solution(mesh):
    return jax.shard_map(
        body,
        mesh=mesh,
        in_specs=(
            P("gx", None, "gy", None),
            P(None, "gy", "gx"),
            P("gy", "gx"),
            P("gy", "gx"),
            P("gy", "gx"),
        ),
        out_specs=P(None, None, "gy", "gx"),
        check_vma=False,
    )
```
